128 devices in a mesh: data: 64 (over z, y, x), model: 2 (over core).
Axes of the slice: x: 4, y: 4, z: 4, core: 2. Of those that a mesh axis runs over, the one named last changes fastest.
Arguments:
- x_t: bfloat16 [128, 128, 768], P('data', 'model')
- x_s: bfloat16 [128, 128, 312], P(('data', 'model'))
- lengths: int32 [128], P(('data', 'model'))
- t_w1: bfloat16 [48, 768, 3072], P(None, None, 'model')
- t_w2: bfloat16 [48, 3072, 768], P(None, 'model')
- t_gain: float32 [48, 768], replicated
- s_w1: bfloat16 [6, 312, 1248], replicated
- s_w2: bfloat16 [6, 1248, 312], replicated
- s_gain1: float32 [6, 312], replicated
- s_gain2: float32 [6, 312], replicated
- s_proj: bfloat16 [6, 312, 768], replicated
Outputs:
- output 1: float32 [], replicated
- output 2: float32 [6, 312, 1248], replicated
- output 3: float32 [6, 1248, 312], replicated
- output 4: float32 [6, 312], replicated
- output 5: float32 [6, 312], replicated
- output 6: float32 [6, 312, 768], replicated
All inputs are finite; a program needn't handle non-finite values.
Results may differ from the reference program's by a relative error of at most 0.00589431.
Values are sent between devices in bfloat16 or wider.
A program may use at most 1 GiB of HBM per device.

```python
import jax
import jax.numpy as jnp
from jax import lax

T_WIDTH = 768
S_WIDTH = 312
SEQ_LEN = 128
S_LAYERS = 6
T_PER_S = 8
ROWS_DEV = 1
N_SEQS = 128

T_LAYERS = S_LAYERS * T_PER_S
T_HIDDEN = 4 * T_WIDTH
S_HIDDEN = 4 * S_WIDTH
RMS_EPS = 1e-6


def draw_lengths(key):
    key_len, key_flag = jax.random.split(key)
    long_len = jax.random.randint(key_len, (N_SEQS,), 1, SEQ_LEN + 1)
    short_flag = jnp.repeat(jax.random.randint(key_flag, (N_SEQS // ROWS_DEV,), 0, 2), ROWS_DEV)
    lengths = jnp.where(short_flag == 1, 1 + long_len // 8, long_len)
    return lengths.at[0].set(SEQ_LEN).astype(jnp.int32)


def setup_inputs(seed: int = 0) -> dict:
    keys = jax.random.split(jax.random.key(seed), 12)

    def draw_normal(key_no, shape, scale):
        return (jax.random.normal(keys[key_no], shape, jnp.float32) * scale).astype(jnp.bfloat16)

    return {
        'x_t': draw_normal(0, (N_SEQS, SEQ_LEN, T_WIDTH), 1.0),
        'x_s': draw_normal(1, (N_SEQS, SEQ_LEN, S_WIDTH), 1.0),
        'lengths': draw_lengths(keys[2]),
        't_w1': draw_normal(3, (T_LAYERS, T_WIDTH, T_HIDDEN), T_WIDTH ** -0.5),
        't_w2': draw_normal(4, (T_LAYERS, T_HIDDEN, T_WIDTH), (T_HIDDEN * T_PER_S) ** -0.5),
        't_gain': jax.random.uniform(keys[5], (T_LAYERS, T_WIDTH), jnp.float32, 0.5, 1.5),
        's_w1': draw_normal(6, (S_LAYERS, S_WIDTH, S_HIDDEN), S_WIDTH ** -0.5),
        's_w2': draw_normal(7, (S_LAYERS, S_HIDDEN, S_WIDTH), S_HIDDEN ** -0.5),
        's_gain1': jax.random.uniform(keys[8], (S_LAYERS, S_WIDTH), jnp.float32, 0.5, 1.5),
        's_gain2': jax.random.uniform(keys[9], (S_LAYERS, S_WIDTH), jnp.float32, 0.5, 1.5),
        's_proj': draw_normal(10, (S_LAYERS, S_WIDTH, T_WIDTH), S_WIDTH ** -0.5),
    }


def rms_gain(hidden, gain):
    wide = hidden.astype(jnp.float32)
    return wide * lax.rsqrt(jnp.mean(wide * wide, axis=-1, keepdims=True) + RMS_EPS) * gain


def snap(values):
    return values + lax.stop_gradient(values.astype(jnp.bfloat16).astype(jnp.float32) - values)


def teacher_layer(hidden, weights):
    w_in, w_out, gain = weights
    normed = rms_gain(hidden, gain).astype(jnp.bfloat16)
    activated = jax.nn.gelu(jnp.dot(normed, w_in, preferred_element_type=jnp.float32)).astype(jnp.bfloat16)
    update = jnp.dot(activated, w_out, preferred_element_type=jnp.float32)
    return (hidden.astype(jnp.float32) + update).astype(jnp.bfloat16), None


def teacher_group(hidden, weights):
    hidden, _ = lax.scan(teacher_layer, hidden, weights)
    return hidden, hidden


def teacher_features(seq_in, t_w1, t_w2, t_gain):
    grouped = (t_w1.reshape(S_LAYERS, T_PER_S, T_WIDTH, T_HIDDEN),
               t_w2.reshape(S_LAYERS, T_PER_S, T_HIDDEN, T_WIDTH),
               t_gain.reshape(S_LAYERS, T_PER_S, T_WIDTH))
    _, features = lax.scan(teacher_group, seq_in, grouped)
    return features


def student_sq_error(params, seq_in, features, valid):
    def block(state, weights):
        w_in, w_out, gain_in, gain_out, w_proj, feature = weights
        normed = snap(rms_gain(state, gain_in))
        activated = snap(jax.nn.gelu(jnp.dot(normed, w_in, preferred_element_type=jnp.float32)))
        state = snap(state + jnp.dot(activated, w_out, preferred_element_type=jnp.float32))
        normed_out = snap(rms_gain(state, gain_out))
        projected = jnp.dot(normed_out, w_proj, preferred_element_type=jnp.float32)
        errors = (projected - feature.astype(jnp.float32)) * valid[:, None]
        return state, jnp.sum(errors * errors)

    w_in, w_out, gain_in, gain_out, w_proj = params
    _, sq_errors = lax.scan(block, seq_in.astype(jnp.float32), (w_in, w_out, gain_in, gain_out, w_proj, features))
    return jnp.sum(sq_errors)


def reference(x_t, x_s, lengths, t_w1, t_w2, t_gain, s_w1, s_w2, s_gain1, s_gain2, s_proj):
    params = (s_w1.astype(jnp.float32), s_w2.astype(jnp.float32), s_gain1, s_gain2, s_proj.astype(jnp.float32))
    positions = jnp.arange(SEQ_LEN)
    loss_grad = jax.value_and_grad(student_sq_error)

    def per_seq(carry, seq_data):
        loss_sum, grad_sum = carry
        xt_seq, xs_seq, seq_len = seq_data
        features = teacher_features(xt_seq, t_w1, t_w2, t_gain)
        valid = (positions < seq_len).astype(jnp.float32)
        seq_loss, seq_grads = loss_grad(params, xs_seq, features, valid)
        return (loss_sum + seq_loss, jax.tree.map(jnp.add, grad_sum, seq_grads)), None

    start = (jnp.zeros((), jnp.float32), jax.tree.map(jnp.zeros_like, params))
    (loss_sum, grad_sum), _ = lax.scan(per_seq, start, (x_t, x_s, lengths))
    inv_count = 1.0 / (S_LAYERS * T_WIDTH * jnp.sum(lengths).astype(jnp.float32))
    return (loss_sum * inv_count, grad_sum[0] * inv_count, grad_sum[1] * inv_count,
            grad_sum[2] * inv_count, grad_sum[3] * inv_count, grad_sum[4] * inv_count)
```

```python
import functools

import jax
import jax.numpy as jnp
from jax import lax
from jax.experimental import pallas as pl
from jax.experimental.pallas import tpu as pltpu
from jax.sharding import PartitionSpec as P

RMS_EPS = 1e-6
ALL_AXES = ('data', 'model')
MESH = pl.DeviceIdType.MESH
GELU_C = 0.7978845608028654
GELU_A = 0.044715
F32 = jnp.float32
BF16 = jnp.bfloat16


def gelu(x):
    return x * (0.5 * (1.0 + jnp.tanh(GELU_C * (x + GELU_A * (x * x * x)))))


def gelu_grad(x):
    sq = x * x
    t = jnp.tanh(GELU_C * (x + GELU_A * (sq * x)))
    return 0.5 * (1.0 + t) + (0.5 * x) * (1.0 - t * t) * (GELU_C * (1.0 + (3.0 * GELU_A) * sq))


def inv_rms(wide):
    return lax.rsqrt(jnp.mean(wide * wide, axis=-1, keepdims=True) + RMS_EPS)


def teacher_kernel(layers, per_group, x_ref, gain_ref, w1_hbm, w2_hbm, feat_ref,
                   xbuf, hbuf, ubuf, part, recv, w1buf, w2buf,
                   x_send, x_recv, w_sem, p_send, p_recv):
    core = lax.axis_index('model')
    peer = {'model': 1 - core}
    seqs, pos, width = hbuf.shape
    hidden = ubuf.shape[1]
    n_out = part.shape[1]
    out_w = part.shape[3]
    slots = w1buf.shape[0]
    half = hidden // 3

    def fetch(layer, slot):
        return (pltpu.make_async_copy(w1_hbm.at[layer], w1buf.at[slot], w_sem.at[slot, 0]),
                pltpu.make_async_copy(w2_hbm.at[layer], w2buf.at[slot], w_sem.at[slot, 1]))

    for layer in range(slots - 1):
        for copy in fetch(layer, layer):
            copy.start()

    barrier = pltpu.get_barrier_semaphore()
    pl.semaphore_signal(barrier, inc=1, device_id=peer, device_id_type=MESH)
    pl.semaphore_wait(barrier, 1)

    x_copy = pltpu.make_async_remote_copy(x_ref, xbuf.at[core], x_send, x_recv, device_id=peer, device_id_type=MESH)
    x_copy.start()
    xbuf[core] = x_ref[...]
    x_copy.wait()
    for seq in range(seqs):
        for c in range(2):
            hbuf[seq, c * (pos // 2):(c + 1) * (pos // 2), :] = xbuf[c, seq]

    def exchange(seq, slot, c):
        return pltpu.make_async_remote_copy(
            part.at[seq, c], recv.at[slot, seq, c], p_send.at[seq, c], p_recv.at[slot, seq, c],
            device_id=peer, device_id_type=MESH)

    def absorb(seq, slot):
        for c in range(n_out):
            exchange(seq, slot, c).wait()
            cols = slice(c * out_w, (c + 1) * out_w)
            update = part[seq, c] + recv[slot, seq, c]
            hbuf[seq, :, cols] = (hbuf[seq, :, cols].astype(F32) + update).astype(BF16)

    def block(layer, _):
        slot = lax.rem(layer, slots)

        @pl.when(layer + (slots - 1) < layers)
        def _():
            for copy in fetch(layer + (slots - 1), lax.rem(layer + (slots - 1), slots)):
                copy.start()

        fetched = fetch(layer, slot)
        for seq in range(seqs):
            @pl.when(layer > 0)
            def _():
                absorb(seq, lax.rem(layer + 1, 2))
            if seq == 0:
                fetched[0].wait()
            wide = hbuf[seq].astype(F32)
            normed = (wide * inv_rms(wide) * gain_ref[layer]).astype(BF16)
            for c in range(3):
                cols = slice(c * half, (c + 1) * half)
                pre = jnp.dot(normed, w1buf[slot, :, cols], preferred_element_type=F32)
                ubuf[:, cols] = gelu(pre).astype(BF16)
            if seq == 0:
                fetched[1].wait()
            act = ubuf[...]
            for c in range(n_out):
                part[seq, c] = jnp.dot(act, w2buf[slot, :, c * out_w:(c + 1) * out_w], preferred_element_type=F32)
                exchange(seq, lax.rem(layer, 2), c).start()

        @pl.when((layer > 0) & (lax.rem(layer, per_group) == 0))
        def _():
            feat_ref[lax.div(layer, per_group) - 1] = hbuf[core]
        return 0

    lax.fori_loop(0, layers, block, 0)
    for seq in range(seqs):
        absorb(seq, (layers - 1) % 2)
    feat_ref[layers // per_group - 1] = hbuf[core]


def teacher(x_t, t_w1, t_w2, t_gain, n_feat):
    layers, width, hidden = t_w1.shape
    seqs, half_pos, _ = x_t.shape
    pos = 2 * half_pos
    slots, n_out = 3, 3
    out_w = width // n_out
    vmem = pl.BlockSpec(memory_space=pltpu.VMEM)
    hbm = pl.BlockSpec(memory_space=pl.ANY)
    return pl.pallas_call(
        functools.partial(teacher_kernel, layers, layers // n_feat),
        out_shape=jax.ShapeDtypeStruct((n_feat, pos, width), BF16),
        in_specs=[vmem, vmem, hbm, hbm],
        out_specs=vmem,
        scratch_shapes=[
            pltpu.VMEM((2, seqs, half_pos, width), BF16),
            pltpu.VMEM((seqs, pos, width), BF16),
            pltpu.VMEM((pos, hidden), BF16),
            pltpu.VMEM((seqs, n_out, pos, out_w), F32),
            pltpu.VMEM((2, seqs, n_out, pos, out_w), F32),
            pltpu.VMEM((slots, width, hidden), BF16),
            pltpu.VMEM((slots, hidden, width), BF16),
            pltpu.SemaphoreType.DMA,
            pltpu.SemaphoreType.DMA,
            pltpu.SemaphoreType.DMA((slots, 2)),
            pltpu.SemaphoreType.DMA((seqs, n_out)),
            pltpu.SemaphoreType.DMA((2, seqs, n_out)),
        ],
        compiler_params=pltpu.CompilerParams(collective_id=0, has_side_effects=True,
                                             vmem_limit_bytes=40 * 1024 * 1024),
        cost_estimate=pl.CostEstimate(flops=4 * seqs * pos * width * hidden * layers,
                                      bytes_accessed=4 * layers * width * hidden, transcendentals=0),
        name='teacher',
    )(x_t, t_gain.reshape(layers, 1, width), t_w1, t_w2)


def dot_tn(a, b):
    return lax.dot_general(a, b, (((0,), (0,)), ((), ())), preferred_element_type=F32)


def dot_nt(a, b):
    return lax.dot_general(a, b, (((1,), (1,)), ((), ())), preferred_element_type=F32)


def rms_back(dy, x, gain):
    r = inv_rms(x)
    xr = x * r
    gdy = dy * gain
    dx = r * (gdy - xr * jnp.mean(gdy * xr, axis=-1, keepdims=True))
    return dx, jnp.sum(dy * xr, axis=0, keepdims=True)


def student_kernel(len_ref, x_ref, feat_ref, w1_ref, w2_ref, g1_ref, g2_ref, proj_ref,
                   gw1_ref, gw2_ref, gg1_ref, gg2_ref, gproj_ref, sq_ref,
                   s_in, s_out, normed_s, pre_s, act_s, dproj_s):
    layers = w1_ref.shape[0]
    pos = x_ref.shape[1]
    valid = (lax.broadcasted_iota(jnp.int32, (pos, 1), 0) < len_ref[0]).astype(F32)

    def forward(layer, carry):
        state, sq = carry
        s_in[layer] = state
        normed = (state * inv_rms(state) * g1_ref[layer]).astype(BF16)
        normed_s[layer] = normed
        pre = jnp.dot(normed, w1_ref[layer], preferred_element_type=F32)
        pre_s[layer] = pre
        act = gelu(pre).astype(BF16)
        act_s[layer] = act
        state = (state + jnp.dot(act, w2_ref[layer], preferred_element_type=F32)).astype(BF16).astype(F32)
        normed_out = (state * inv_rms(state) * g2_ref[layer]).astype(BF16)
        err = (jnp.dot(normed_out, proj_ref[layer], preferred_element_type=F32) - feat_ref[layer].astype(F32)) * valid
        sq = sq + jnp.sum(jnp.sum(err * err, axis=0, keepdims=True), axis=1, keepdims=True)
        d_err = err.astype(BF16)
        gproj_ref[layer] = dot_tn(normed_out, d_err)
        d_out = dot_nt(d_err, proj_ref[layer])
        dx, dg = rms_back(d_out, state, g2_ref[layer])
        dproj_s[layer] = dx
        gg2_ref[layer] = dg
        return state, sq

    _, sq = lax.fori_loop(0, layers, forward, (x_ref[0].astype(F32), jnp.zeros((1, 1), F32)))
    sq_ref[...] = sq

    def backward(step, d_state):
        layer = layers - 1 - step
        d_state = d_state + dproj_s[layer]
        d_update = d_state.astype(BF16)
        gw2_ref[layer] = dot_tn(act_s[layer], d_update)
        d_act = dot_nt(d_update, w2_ref[layer])
        d_pre = (d_act * gelu_grad(pre_s[layer])).astype(BF16)
        gw1_ref[layer] = dot_tn(normed_s[layer], d_pre)
        d_norm = dot_nt(d_pre, w1_ref[layer])
        dx, dg = rms_back(d_norm, s_in[layer], g1_ref[layer])
        gg1_ref[layer] = dg
        return d_state + dx

    lax.fori_loop(0, layers, backward, jnp.zeros(s_in.shape[1:], F32))


def student(x_s, lengths, feats, s_w1, s_w2, s_gain1, s_gain2, s_proj):
    layers, width, hidden = s_w1.shape
    t_width = s_proj.shape[2]
    pos = x_s.shape[1]
    vmem = pl.BlockSpec(memory_space=pltpu.VMEM)
    smem = pl.BlockSpec(memory_space=pltpu.SMEM)
    return pl.pallas_call(
        student_kernel,
        out_shape=(jax.ShapeDtypeStruct((layers, width, hidden), F32),
                   jax.ShapeDtypeStruct((layers, hidden, width), F32),
                   jax.ShapeDtypeStruct((layers, 1, width), F32),
                   jax.ShapeDtypeStruct((layers, 1, width), F32),
                   jax.ShapeDtypeStruct((layers, width, t_width), F32),
                   jax.ShapeDtypeStruct((1, 1), F32)),
        in_specs=[smem] + [vmem] * 7,
        out_specs=[vmem] * 6,
        scratch_shapes=[
            pltpu.VMEM((layers, pos, width), F32),
            pltpu.VMEM((1, 1), F32),
            pltpu.VMEM((layers, pos, width), BF16),
            pltpu.VMEM((layers, pos, hidden), F32),
            pltpu.VMEM((layers, pos, hidden), BF16),
            pltpu.VMEM((layers, pos, width), F32),
        ],
        compiler_params=pltpu.CompilerParams(vmem_limit_bytes=63 * 1024 * 1024),
        name='student',
    )(lengths, x_s, feats, s_w1, s_w2, s_gain1.reshape(layers, 1, width), s_gain2.reshape(layers, 1, width), s_proj)


def solution(mesh):
    def body(x_t, x_s, lengths, t_w1, t_w2, t_gain, s_w1, s_w2, s_gain1, s_gain2, s_proj):
        n_feat = s_w1.shape[0]
        feats = teacher(x_t, t_w1, t_w2, t_gain, n_feat)
        gw1, gw2, gg1, gg2, gproj, sq = student(x_s, lengths, feats, s_w1, s_w2, s_gain1, s_gain2, s_proj)
        tokens = jnp.sum(lengths).astype(F32)
        gw1, gw2, gproj, gg1, gg2, sq, tokens = lax.psum((gw1, gw2, gproj, gg1, gg2, sq, tokens), ALL_AXES)
        inv = 1.0 / (n_feat * x_t.shape[2] * tokens)
        two = 2.0 * inv
        shape = s_gain1.shape
        return (sq[0, 0] * inv, gw1 * two, gw2 * two, gg1.reshape(shape) * two, gg2.reshape(shape) * two, gproj * two)

    in_specs = (P('data', 'model', None), P(ALL_AXES, None, None), P(ALL_AXES),
                P(None, None, 'model'), P(None, 'model', None), P(), P(), P(), P(), P(), P())
    out_specs = (P(), P(), P(), P(), P(), P())
    return jax.shard_map(body, mesh=mesh, in_specs=in_specs, out_specs=out_specs, check_vma=False)
```

```python
import functools

import jax
import jax.numpy as jnp
from jax import lax
from jax.experimental import pallas as pl
from jax.experimental.pallas import tpu as pltpu
from jax.sharding import PartitionSpec as P

RMS_EPS = 1e-6
ALL_AXES = ('data', 'model')
MESH = pl.DeviceIdType.MESH
GELU_C = 0.7978845608028654
GELU_A = 0.044715
F32 = jnp.float32
BF16 = jnp.bfloat16


def gelu(x):
    return x * (0.5 * (1.0 + jnp.tanh(GELU_C * (x + GELU_A * (x * x * x)))))


def gelu_grad(x):
    sq = x * x
    t = jnp.tanh(GELU_C * (x + GELU_A * (sq * x)))
    return 0.5 * (1.0 + t) + (0.5 * x) * (1.0 - t * t) * (GELU_C * (1.0 + (3.0 * GELU_A) * sq))


def inv_rms(wide):
    return lax.rsqrt(jnp.mean(wide * wide, axis=-1, keepdims=True) + RMS_EPS)


def teacher_kernel(layers, per_group, x_ref, gain_ref, w1_hbm, w2_hbm, feat_ref,
                   xbuf, hbuf, ubuf, part, recv, w1buf, w2buf,
                   x_send, x_recv, w_sem, p_send, p_recv):
    core = lax.axis_index('model')
    peer = {'model': 1 - core}
    seqs, pos, width = hbuf.shape
    hidden = ubuf.shape[1]
    n_out = part.shape[1]
    out_w = part.shape[3]
    slots = w1buf.shape[0]
    half = hidden // 3

    def fetch(layer, slot):
        return (pltpu.make_async_copy(w1_hbm.at[layer], w1buf.at[slot], w_sem.at[slot, 0]),
                pltpu.make_async_copy(w2_hbm.at[layer], w2buf.at[slot], w_sem.at[slot, 1]))

    for layer in range(slots - 1):
        for copy in fetch(layer, layer):
            copy.start()

    barrier = pltpu.get_barrier_semaphore()
    pl.semaphore_signal(barrier, inc=1, device_id=peer, device_id_type=MESH)
    pl.semaphore_wait(barrier, 1)

    x_copy = pltpu.make_async_remote_copy(x_ref, xbuf.at[core], x_send, x_recv, device_id=peer, device_id_type=MESH)
    x_copy.start()
    xbuf[core] = x_ref[...]
    x_copy.wait()
    for seq in range(seqs):
        for c in range(2):
            hbuf[seq, c * (pos // 2):(c + 1) * (pos // 2), :] = xbuf[c, seq]

    def exchange(seq, slot, c):
        return pltpu.make_async_remote_copy(
            part.at[seq, c], recv.at[slot, seq, c], p_send.at[seq, c], p_recv.at[slot, seq, c],
            device_id=peer, device_id_type=MESH)

    def absorb(seq, slot):
        for c in range(n_out):
            exchange(seq, slot, c).wait()
            cols = slice(c * out_w, (c + 1) * out_w)
            update = part[seq, c] + recv[slot, seq, c]
            hbuf[seq, :, cols] = (hbuf[seq, :, cols].astype(F32) + update).astype(BF16)

    def block(layer, _):
        slot = lax.rem(layer, slots)

        @pl.when(layer + (slots - 1) < layers)
        def _():
            for copy in fetch(layer + (slots - 1), lax.rem(layer + (slots - 1), slots)):
                copy.start()

        fetched = fetch(layer, slot)
        for seq in range(seqs):
            @pl.when(layer > 0)
            def _():
                absorb(seq, lax.rem(layer + 1, 2))
            if seq == 0:
                fetched[0].wait()
            wide = hbuf[seq].astype(F32)
            normed = (wide * inv_rms(wide) * gain_ref[pl.ds(layer, 1), :]).astype(BF16)
            for c in range(3):
                cols = slice(c * half, (c + 1) * half)
                pre = jnp.dot(normed, w1buf[slot, :, cols], preferred_element_type=F32)
                ubuf[:, cols] = gelu(pre).astype(BF16)
            if seq == 0:
                fetched[1].wait()
            act = ubuf[...]
            for c in range(n_out):
                part[seq, c] = jnp.dot(act, w2buf[slot, :, c * out_w:(c + 1) * out_w], preferred_element_type=F32)
                exchange(seq, lax.rem(layer, 2), c).start()

        @pl.when((layer > 0) & (lax.rem(layer, per_group) == 0))
        def _():
            feat_ref[lax.div(layer, per_group) - 1] = hbuf[core]
        return 0

    lax.fori_loop(0, layers, block, 0)
    for seq in range(seqs):
        absorb(seq, (layers - 1) % 2)
    feat_ref[layers // per_group - 1] = hbuf[core]


def teacher(x_t, t_w1, t_w2, t_gain, n_feat):
    layers, width, hidden = t_w1.shape
    seqs, half_pos, _ = x_t.shape
    pos = 2 * half_pos
    slots, n_out = 3, 3
    out_w = width // n_out
    vmem = pl.BlockSpec(memory_space=pltpu.VMEM)
    hbm = pl.BlockSpec(memory_space=pl.ANY)
    return pl.pallas_call(
        functools.partial(teacher_kernel, layers, layers // n_feat),
        out_shape=jax.ShapeDtypeStruct((n_feat, pos, width), BF16),
        in_specs=[vmem, vmem, hbm, hbm],
        out_specs=vmem,
        scratch_shapes=[
            pltpu.VMEM((2, seqs, half_pos, width), BF16),
            pltpu.VMEM((seqs, pos, width), BF16),
            pltpu.VMEM((pos, hidden), BF16),
            pltpu.VMEM((seqs, n_out, pos, out_w), F32),
            pltpu.VMEM((2, seqs, n_out, pos, out_w), F32),
            pltpu.VMEM((slots, width, hidden), BF16),
            pltpu.VMEM((slots, hidden, width), BF16),
            pltpu.SemaphoreType.DMA,
            pltpu.SemaphoreType.DMA,
            pltpu.SemaphoreType.DMA((slots, 2)),
            pltpu.SemaphoreType.DMA((seqs, n_out)),
            pltpu.SemaphoreType.DMA((2, seqs, n_out)),
        ],
        compiler_params=pltpu.CompilerParams(collective_id=0, has_side_effects=True,
                                             vmem_limit_bytes=40 * 1024 * 1024),
        cost_estimate=pl.CostEstimate(flops=4 * seqs * pos * width * hidden * layers,
                                      bytes_accessed=4 * layers * width * hidden, transcendentals=0),
        name='teacher',
    )(x_t, t_gain, t_w1, t_w2)


def dot_tn(a, b):
    return lax.dot_general(a, b, (((0,), (0,)), ((), ())), preferred_element_type=F32)


def dot_nt(a, b):
    return lax.dot_general(a, b, (((1,), (1,)), ((), ())), preferred_element_type=F32)


def rms_back(dy, x, gain):
    r = inv_rms(x)
    xr = x * r
    gdy = dy * gain
    dx = r * (gdy - xr * jnp.mean(gdy * xr, axis=-1, keepdims=True))
    return dx, jnp.sum(dy * xr, axis=0, keepdims=True)


TILES = 1024
ROW_TILES = 39
W2_AT, W1_AT, SMALL_AT = 234, 624, 1014
SQ_TILE, COUNT_TILE = SMALL_AT + 6, SMALL_AT + 7
PARTS = ((0, W2_AT), (W2_AT, W1_AT - W2_AT), (W1_AT, TILES - W1_AT))


def store_tiles(ref, idx, start, value):
    width = value.shape[1]
    for ct in range(-(-width // 128)):
        lanes = min(128, width - ct * 128)
        piece = value[:, ct * 128:ct * 128 + lanes]
        if lanes < 128:
            piece = jnp.concatenate([piece, jnp.zeros((piece.shape[0], 128 - lanes), F32)], axis=1)
        ref[idx, start + ct * ROW_TILES:start + (ct + 1) * ROW_TILES] = piece.reshape(ROW_TILES, 8, 128)


def store_row(ref, idx, start, row):
    width = row.shape[1]
    for ct in range(-(-width // 128)):
        lanes = min(128, width - ct * 128)
        piece = row[:, ct * 128:ct * 128 + lanes]
        if lanes < 128:
            piece = jnp.concatenate([piece, jnp.zeros((1, 128 - lanes), F32)], axis=1)
        ref[idx, start + ct] = jnp.broadcast_to(piece, (8, 128))


def student_kernel(len_ref, x_ref, feat_ref, w1_ref, w2_ref, g1_ref, g2_ref, proj_ref, out_hbm,
                   grad, recv, s_in, normed_s, pre_s, act_s, dproj_s, send_sem, recv_sem, out_sem):
    core = lax.axis_index('model')
    peer = {'model': 1 - core}
    layers = w1_ref.shape[0]
    pairs = layers // 2
    pos = x_ref.shape[2]
    barrier = pltpu.get_barrier_semaphore()
    pl.semaphore_signal(barrier, inc=1, device_id=peer, device_id_type=MESH)
    pl.semaphore_wait(barrier, 1)
    valid = (lax.broadcasted_iota(jnp.int32, (pos, 1), 0) < len_ref[0]).astype(F32)
    tokens = jnp.broadcast_to(len_ref[0].astype(F32), (8, 128))

    def send(pair, part):
        start, size = PARTS[part]
        return pltpu.make_async_remote_copy(
            grad.at[pairs + pair, pl.ds(start, size)], recv.at[pair, pl.ds(start, size)],
            send_sem.at[pair, part], recv_sem.at[pair, part], device_id=peer, device_id_type=MESH)

    def place(layer):
        pair = lax.div(layer, 2)
        mine = lax.rem(layer, 2) == core
        return pair, mine, jnp.where(mine, pair, pairs + pair)

    def forward(layer, state):
        pair, mine, idx = place(layer)
        s_in[layer] = state
        normed = (state * inv_rms(state) * g1_ref[pl.ds(layer, 1), :]).astype(BF16)
        normed_s[layer] = normed
        pre = jnp.dot(normed, w1_ref[layer], preferred_element_type=F32)
        pre_s[layer] = pre
        act = gelu(pre).astype(BF16)
        act_s[layer] = act
        state = (state + dot_nt(act, w2_ref[layer])).astype(BF16).astype(F32)
        normed_out = (state * inv_rms(state) * g2_ref[pl.ds(layer, 1), :]).astype(BF16)
        err = (jnp.dot(normed_out, proj_ref[layer], preferred_element_type=F32) - feat_ref[layer].astype(F32)) * valid
        sq = jnp.sum(jnp.sum(err * err, axis=0, keepdims=True), axis=1, keepdims=True)
        d_err = err.astype(BF16)
        store_tiles(grad, idx, 0, dot_tn(normed_out, d_err))

        @pl.when(jnp.logical_not(mine))
        def _():
            send(pair, 0).start()

        dx, dg = rms_back(dot_nt(d_err, proj_ref[layer]), state, g2_ref[pl.ds(layer, 1), :])
        dproj_s[layer] = dx
        store_row(grad, idx, SMALL_AT + 3, dg)
        grad[idx, SQ_TILE] = jnp.broadcast_to(sq, (8, 128))
        grad[idx, COUNT_TILE] = tokens
        for spare in range(COUNT_TILE + 1, TILES):
            grad[idx, spare] = jnp.zeros((8, 128), F32)
        return state

    lax.fori_loop(0, layers, forward, x_ref[0].astype(F32).T)

    def backward(step, d_state):
        layer = layers - 1 - step
        pair, mine, idx = place(layer)
        d_state = d_state + dproj_s[layer]
        d_update = d_state.astype(BF16)
        store_tiles(grad, idx, W2_AT, dot_tn(d_update, act_s[layer]))

        @pl.when(jnp.logical_not(mine))
        def _():
            send(pair, 1).start()

        d_act = jnp.dot(d_update, w2_ref[layer], preferred_element_type=F32)
        d_pre = (d_act * gelu_grad(pre_s[layer])).astype(BF16)
        dx, dg = rms_back(dot_nt(d_pre, w1_ref[layer]), s_in[layer], g1_ref[pl.ds(layer, 1), :])
        store_row(grad, idx, SMALL_AT, dg)
        store_tiles(grad, idx, W1_AT, dot_tn(normed_s[layer], d_pre))

        @pl.when(jnp.logical_not(mine))
        def _():
            send(pair, 2).start()

        return d_state + dx

    lax.fori_loop(0, layers, backward, jnp.zeros(s_in.shape[1:], F32))

    def out_copy(pair):
        return pltpu.make_async_copy(grad.at[pair], out_hbm.at[pair], out_sem.at[pair])

    for pair in reversed(range(pairs)):
        for part in range(3):
            send(pair, part).wait_recv()
            start, size = PARTS[part]
            span = pl.ds(start, size)
            grad[pair, span] = grad[pair, span] + recv[pair, span]
        out_copy(pair).start()
    for pair in range(pairs):
        for part in range(3):
            send(pair, part).wait_send()
        out_copy(pair).wait()


def student(x_s, lengths, feats, s_w1, s_w2t, s_gain1, s_gain2, s_proj):
    layers, width, hidden = s_w1.shape
    pos = x_s.shape[2]
    vmem = pl.BlockSpec(memory_space=pltpu.VMEM)
    return pl.pallas_call(
        student_kernel,
        out_shape=jax.ShapeDtypeStruct((layers // 2, TILES, 8, 128), F32),
        in_specs=[pl.BlockSpec(memory_space=pltpu.SMEM)] + [vmem] * 7,
        out_specs=pl.BlockSpec(memory_space=pl.ANY),
        scratch_shapes=[
            pltpu.VMEM((layers, TILES, 8, 128), F32),
            pltpu.VMEM((layers // 2, TILES, 8, 128), F32),
            pltpu.VMEM((layers, pos, width), F32),
            pltpu.VMEM((layers, pos, width), BF16),
            pltpu.VMEM((layers, pos, hidden), F32),
            pltpu.VMEM((layers, pos, hidden), BF16),
            pltpu.VMEM((layers, pos, width), F32),
            pltpu.SemaphoreType.DMA((layers // 2, 3)),
            pltpu.SemaphoreType.DMA((layers // 2, 3)),
            pltpu.SemaphoreType.DMA((layers // 2,)),
        ],
        compiler_params=pltpu.CompilerParams(collective_id=1, has_side_effects=True,
                                             vmem_limit_bytes=67_043_328),
        name='student',
    )(lengths, x_s, feats, s_w1, s_w2t, s_gain1, s_gain2, s_proj)


def reduce_kernel(side, g_hbm, out_hbm, data, full, near, far,
                  load_sem, rs_send, rs_recv, ag_send, ag_recv, own_sem, d2d_send, d2d_recv):
    core = lax.axis_index('model')
    chip = lax.axis_index('data')
    peer = {'model': 1 - core}
    colors = data.shape[0]
    coord = [lax.rem(chip, side), lax.rem(lax.div(chip, side), side), lax.div(chip, side * side)]

    def shifted(axis, by):
        moved = list(coord)
        moved[axis] = lax.rem(coord[axis] + by, side)
        return {'data': (moved[2] * side + moved[1]) * side + moved[0]}

    def load(c, a):
        span = pl.ds(a * 256, 256)
        return pltpu.make_async_copy(g_hbm.at[c, span], data.at[c, span], load_sem.at[c, a])

    for a in range(4):
        for c in range(colors):
            load(c, a).start()

    barrier = pltpu.get_barrier_semaphore()
    pl.semaphore_signal(barrier, inc=1, device_id=peer, device_id_type=MESH)
    for axis in range(3):
        for by in (1, side - 1):
            pl.semaphore_signal(barrier, inc=1, device_id=shifted(axis, by), device_id_type=MESH)
    pl.semaphore_wait(barrier, 7)

    for a in range(4):
        for c in range(colors):
            load(c, a).wait()

    plus = [shifted(axis, 1) for axis in range(3)]
    minus = [shifted(axis, side - 1) for axis in range(3)]
    sent = []
    base = [0] * colors
    bases = []
    near_at, far_at = 0, 0
    size = 256

    for phase in range(3):
        half = size // 2
        bases.append(list(base))

        def chunk(c, by):
            axis = (c + phase) % 3
            return base[c] + lax.rem(coord[axis] + by, side) * size

        def push(c, kind, src, dst, upward):
            axis = (c + phase) % 3
            copy = pltpu.make_async_remote_copy(
                src, dst, rs_send.at[c, phase, kind], rs_recv.at[c, phase, kind],
                device_id=plus[axis] if upward else minus[axis], device_id_type=MESH)
            copy.start()
            sent.append(copy)
            return copy

        first, early, late = {}, {}, {}
        for c in range(colors):
            opp, nxt, prv = chunk(c, 2), chunk(c, 1), chunk(c, 3)
            first[c] = (
                push(c, 0, data.at[c, pl.ds(opp, half)], near.at[c, 0, pl.ds(near_at, half)], True),
                push(c, 1, data.at[c, pl.ds(opp + half, half)], near.at[c, 1, pl.ds(near_at, half)], False))
            early[c] = (
                push(c, 2, data.at[c, pl.ds(nxt + half, half)], far.at[c, 0, pl.ds(far_at + half, half)], True),
                push(c, 3, data.at[c, pl.ds(prv, half)], far.at[c, 1, pl.ds(far_at, half)], False))
        for c in range(colors):
            nxt, prv = chunk(c, 1), chunk(c, 3)
            first[c][0].wait_recv()
            span = pl.ds(nxt, half)
            data[c, span] = data[c, span] + near[c, 0, pl.ds(near_at, half)]
            up = push(c, 4, data.at[c, span], far.at[c, 0, pl.ds(far_at, half)], True)
            first[c][1].wait_recv()
            span = pl.ds(prv + half, half)
            data[c, span] = data[c, span] + near[c, 1, pl.ds(near_at, half)]
            down = push(c, 5, data.at[c, span], far.at[c, 1, pl.ds(far_at + half, half)], False)
            late[c] = (up, down)
        for c in range(colors):
            for copy in early[c] + late[c]:
                copy.wait_recv()
            mine = pl.ds(chunk(c, 0), size)
            both = far[c, 0, pl.ds(far_at, size)] + far[c, 1, pl.ds(far_at, size)]
            if phase < 2:
                data[c, mine] = data[c, mine] + both
            else:
                full[c, mine] = data[c, mine] + both
        base = [chunk(c, 0) for c in range(colors)]
        near_at, far_at, size = near_at + half, far_at + size, half // 2

    emitted = []

    def emit(c, slot, start, count):
        layer = 2 * c + core
        span = pl.ds(start, count)
        own = pltpu.make_async_copy(full.at[c, span], out_hbm.at[layer, span], own_sem.at[c, slot])
        own.start()
        across = pltpu.make_async_remote_copy(
            full.at[c, span], out_hbm.at[layer, span], d2d_send.at[c, slot], d2d_recv.at[c, slot],
            device_id=peer, device_id_type=MESH)
        across.start()
        emitted.append((own, across))

    for phase in (2, 1, 0):
        size = 256 // 4 ** phase
        half = size // 2
        base = bases[phase]
        last = phase == 0

        def part(c, by, upper):
            axis = (c + phase) % 3
            return base[c] + lax.rem(coord[axis] + by, side) * size + (half if upper else 0)

        def spread(c, kind, start, upward):
            axis = (c + phase) % 3
            span = pl.ds(start, half)
            copy = pltpu.make_async_remote_copy(
                full.at[c, span], full.at[c, span], ag_send.at[c, phase, kind], ag_recv.at[c, phase, kind],
                device_id=plus[axis] if upward else minus[axis], device_id_type=MESH)
            copy.start()
            sent.append(copy)
            return copy

        direct, passed = {}, {}
        for c in range(colors):
            low, high = part(c, 0, False), part(c, 0, True)
            direct[c] = (spread(c, 0, low, True), spread(c, 1, high, False),
                         spread(c, 2, high, True), spread(c, 3, low, False))
            if last:
                emit(c, 0, low, size)
        for c in range(colors):
            direct[c][0].wait_recv()
            up = spread(c, 4, part(c, 3, False), True)
            direct[c][1].wait_recv()
            down = spread(c, 5, part(c, 1, True), False)
            passed[c] = (up, down)
            if last:
                emit(c, 1, part(c, 3, False), half)
                emit(c, 2, part(c, 1, True), half)
        for c in range(colors):
            direct[c][2].wait_recv()
            if last:
                emit(c, 3, part(c, 3, True), half)
            direct[c][3].wait_recv()
            if last:
                emit(c, 4, part(c, 1, False), half)
        for c in range(colors):
            passed[c][0].wait_recv()
            if last:
                emit(c, 5, part(c, 2, False), half)
            passed[c][1].wait_recv()
            if last:
                emit(c, 6, part(c, 2, True), half)

    for copy in sent:
        copy.wait_send()
    for own, across in emitted:
        own.wait()
        across.wait()


def reduce_all(grads, side):
    colors = grads.shape[0]
    hbm = pl.BlockSpec(memory_space=pl.ANY)
    return pl.pallas_call(
        functools.partial(reduce_kernel, side),
        out_shape=jax.ShapeDtypeStruct((2 * colors, TILES, 8, 128), F32),
        in_specs=[hbm],
        out_specs=hbm,
        scratch_shapes=[
            pltpu.VMEM((colors, TILES, 8, 128), F32),
            pltpu.VMEM((colors, TILES, 8, 128), F32),
            pltpu.VMEM((colors, 2, 168, 8, 128), F32),
            pltpu.VMEM((colors, 2, 336, 8, 128), F32),
            pltpu.SemaphoreType.DMA((colors, 4)),
            pltpu.SemaphoreType.DMA((colors, 3, 6)),
            pltpu.SemaphoreType.DMA((colors, 3, 6)),
            pltpu.SemaphoreType.DMA((colors, 3, 6)),
            pltpu.SemaphoreType.DMA((colors, 3, 6)),
            pltpu.SemaphoreType.DMA((colors, 7)),
            pltpu.SemaphoreType.DMA((colors, 7)),
            pltpu.SemaphoreType.DMA((colors, 7)),
        ],
        compiler_params=pltpu.CompilerParams(collective_id=2, has_side_effects=True,
                                             vmem_limit_bytes=56 * 1024 * 1024),
        name='reduce_all',
    )(grads)


def finish_kernel(terms, flat_ref, loss_ref, gw1_ref, gw2_ref, gg1_ref, gg2_ref, gproj_ref):
    layer = pl.program_id(0)
    inv = 1.0 / (terms * flat_ref[0, COUNT_TILE, 0:1, 0:1])
    two = 2.0 * inv

    def unpack(ref, start, rows):
        width = ref.shape[2]
        for ct in range(-(-width // 128)):
            lanes = min(128, width - ct * 128)
            piece = flat_ref[0, start + ct * ROW_TILES:start + (ct + 1) * ROW_TILES].reshape(rows, 128) * two
            ref[0, :, ct * 128:ct * 128 + lanes] = piece[:, :lanes]

    unpack(gproj_ref, 0, gproj_ref.shape[1])
    unpack(gw2_ref, W2_AT, gw2_ref.shape[1])
    unpack(gw1_ref, W1_AT, gw1_ref.shape[1])
    for ref, start in ((gg1_ref, SMALL_AT), (gg2_ref, SMALL_AT + 3)):
        width = ref.shape[1]
        for ct in range(-(-width // 128)):
            lanes = min(128, width - ct * 128)
            cols = slice(ct * 128, ct * 128 + lanes)
            row = flat_ref[0, start + ct, 0:1, 0:lanes] * two
            here = lax.broadcasted_iota(jnp.int32, (ref.shape[0], lanes), 0) == layer
            ref[:, cols] = jnp.where(here, row, ref[:, cols])

    @pl.when(layer == 0)
    def _():
        loss_ref[...] = jnp.zeros_like(loss_ref)

    loss_ref[...] += flat_ref[0, SQ_TILE, 0:1, 0:1] * inv


def finish(flat, width, hidden, t_width):
    layers = flat.shape[0]
    per_layer = lambda a, b: pl.BlockSpec((1, a, b), lambda l: (l, 0, 0))
    whole = lambda a, b: pl.BlockSpec((a, b), lambda l: (0, 0))
    return pl.pallas_call(
        functools.partial(finish_kernel, float(layers * t_width)),
        grid=(layers,),
        out_shape=(jax.ShapeDtypeStruct((1, 1), F32),
                   jax.ShapeDtypeStruct((layers, width, hidden), F32),
                   jax.ShapeDtypeStruct((layers, width, hidden), F32),
                   jax.ShapeDtypeStruct((layers, width), F32),
                   jax.ShapeDtypeStruct((layers, width), F32),
                   jax.ShapeDtypeStruct((layers, width, t_width), F32)),
        in_specs=[pl.BlockSpec((1, TILES, 8, 128), lambda l: (l, 0, 0, 0))],
        out_specs=(whole(1, 1), per_layer(width, hidden), per_layer(width, hidden),
                   whole(layers, width), whole(layers, width), per_layer(width, t_width)),
        compiler_params=pltpu.CompilerParams(vmem_limit_bytes=48 * 1024 * 1024),
        name='finish',
    )(flat)


def solution(mesh):
    side = round(mesh.shape['data'] ** (1 / 3))

    def body(x_t, x_s, lengths, t_w1, t_w2, t_gain, s_w1, s_w2, s_gain1, s_gain2, s_proj):
        layers, width, hidden = s_w1.shape
        feats = teacher(x_t, t_w1, t_w2, t_gain, layers)
        grads = student(jnp.swapaxes(x_s, 1, 2), lengths, feats, s_w1, jnp.swapaxes(s_w2, 1, 2),
                        s_gain1, s_gain2, s_proj)
        flat = reduce_all(grads, side)
        loss, gw1, gw2, gg1, gg2, gproj = finish(flat, width, hidden, x_t.shape[2])
        return loss[0, 0], gw1, jnp.swapaxes(gw2, 1, 2), gg1, gg2, gproj

    in_specs = (P('data', 'model', None), P(ALL_AXES, None, None), P(ALL_AXES),
                P(None, None, 'model'), P(None, 'model', None), P(), P(), P(), P(), P(), P())
    out_specs = (P(), P(), P(), P(), P(), P())
    return jax.shard_map(body, mesh=mesh, in_specs=in_specs, out_specs=out_specs, check_vma=False)
```

```python
import functools

import jax
import jax.numpy as jnp
from jax import lax
from jax.experimental import pallas as pl
from jax.experimental.pallas import tpu as pltpu
from jax.sharding import PartitionSpec as P

RMS_EPS = 1e-6
ALL_AXES = ('data', 'model')
MESH = pl.DeviceIdType.MESH
GELU_C = 0.7978845608028654
GELU_A = 0.044715
F32 = jnp.float32
BF16 = jnp.bfloat16


def gelu(x):
    half = 0.5 * x
    return half + half * jnp.tanh(x * (GELU_C + (GELU_C * GELU_A) * (x * x)))


def gelu_grad(x):
    sq = x * x
    t = jnp.tanh(GELU_C * (x + GELU_A * (sq * x)))
    return 0.5 * (1.0 + t) + (0.5 * x) * (1.0 - t * t) * (GELU_C * (1.0 + (3.0 * GELU_A) * sq))


def inv_rms(wide):
    return lax.rsqrt(jnp.mean(wide * wide, axis=-1, keepdims=True) + RMS_EPS)


def teacher_kernel(layers, per_group, spans, k_chunks, x_ref, gain_ref, w1_hbm, w2_hbm, feat_ref,
                   xbuf, hbuf, part, recv, w1buf, w2buf,
                   x_send, x_recv, w_sem, p_send, p_recv):
    core = lax.axis_index('model')
    peer = {'model': 1 - core}
    seqs, pos, width = hbuf.shape
    slots, _, hidden = w1buf.shape
    blocks, out_w = part.shape[1], part.shape[3]
    step = hidden // k_chunks

    def fetch(layer, slot):
        return (pltpu.make_async_copy(w1_hbm.at[layer], w1buf.at[slot], w_sem.at[slot, 0]),
                pltpu.make_async_copy(w2_hbm.at[layer], w2buf.at[slot], w_sem.at[slot, 1]))

    for layer in range(slots - 1):
        for copy in fetch(layer, layer):
            copy.start()

    barrier = pltpu.get_barrier_semaphore()
    pl.semaphore_signal(barrier, inc=1, device_id=peer, device_id_type=MESH)
    part[...] = jnp.zeros(part.shape, F32)
    recv[1] = jnp.zeros(recv.shape[1:], F32)
    xbuf[core] = x_ref[...]
    pl.semaphore_wait(barrier, 1)

    x_copy = pltpu.make_async_remote_copy(x_ref, xbuf.at[core], x_send, x_recv, device_id=peer, device_id_type=MESH)
    x_copy.start()
    x_copy.wait()
    for seq in range(seqs):
        for c in range(2):
            hbuf[seq, c * (pos // 2):(c + 1) * (pos // 2), :] = xbuf[c, seq]

    def exchange(seq, slot, k):
        span = pl.ds(*spans[k])
        return pltpu.make_async_remote_copy(
            part.at[seq, span], recv.at[slot, seq, span], p_send.at[seq, k], p_recv.at[slot, seq, k],
            device_id=peer, device_id_type=MESH)

    def absorb(seq, slot):
        update = jnp.concatenate([part[seq, b] + recv[slot, seq, b] for b in range(blocks)], axis=1)
        state = (hbuf[seq].astype(F32) + update).astype(BF16)
        hbuf[seq] = state
        return state.astype(F32)

    def block(layer, _):
        slot = lax.rem(layer, slots)

        @pl.when(layer + (slots - 1) < layers)
        def _():
            for copy in fetch(layer + (slots - 1), lax.rem(layer + (slots - 1), slots)):
                copy.start()

        for seq in range(seqs):
            old = lax.rem(layer + 1, 2)
            if seq == 0:
                for copy in fetch(layer, slot):
                    copy.wait()

            @pl.when(layer > 0)
            def _():
                for k in range(len(spans)):
                    exchange(seq, old, k).wait()

            wide = absorb(seq, old)
            normed = (wide * inv_rms(wide) * gain_ref[pl.ds(layer, 1), :]).astype(BF16)
            acc = [None] * len(spans)
            for c in range(k_chunks):
                pre = jnp.dot(normed, w1buf[slot, :, c * step:(c + 1) * step], preferred_element_type=F32)
                act = gelu(pre).astype(BF16)
                for k, (first, count) in enumerate(spans):
                    cols = slice(first * out_w, (first + count) * out_w)
                    term = jnp.dot(act, w2buf[slot, c * step:(c + 1) * step, cols], preferred_element_type=F32)
                    acc[k] = term if acc[k] is None else acc[k] + term
                    if c == k_chunks - 1:
                        for b in range(count):
                            part[seq, first + b] = acc[k][:, b * out_w:(b + 1) * out_w]
                        exchange(seq, lax.rem(layer, 2), k).start()

        @pl.when((layer > 0) & (lax.rem(layer, per_group) == 0))
        def _():
            feat_ref[lax.div(layer, per_group) - 1] = hbuf[core]
        return 0

    lax.fori_loop(0, layers, block, 0)
    for seq in range(seqs):
        for k in range(len(spans)):
            exchange(seq, (layers - 1) % 2, k).wait()
        absorb(seq, (layers - 1) % 2)
    feat_ref[layers // per_group - 1] = hbuf[core]


def teacher(x_t, t_w1, t_w2, t_gain, n_feat):
    layers, width, hidden = t_w1.shape
    seqs, half_pos, _ = x_t.shape
    pos = 2 * half_pos
    slots, blocks = 3, 3
    out_w = width // blocks
    spans = ((0, 1), (1, 2))
    vmem = pl.BlockSpec(memory_space=pltpu.VMEM)
    hbm = pl.BlockSpec(memory_space=pl.ANY)
    return pl.pallas_call(
        functools.partial(teacher_kernel, layers, layers // n_feat, spans, 1),
        out_shape=jax.ShapeDtypeStruct((n_feat, pos, width), BF16),
        in_specs=[vmem, vmem, hbm, hbm],
        out_specs=vmem,
        scratch_shapes=[
            pltpu.VMEM((2, seqs, half_pos, width), BF16),
            pltpu.VMEM((seqs, pos, width), BF16),
            pltpu.VMEM((seqs, blocks, pos, out_w), F32),
            pltpu.VMEM((2, seqs, blocks, pos, out_w), F32),
            pltpu.VMEM((slots, width, hidden), BF16),
            pltpu.VMEM((slots, hidden, width), BF16),
            pltpu.SemaphoreType.DMA,
            pltpu.SemaphoreType.DMA,
            pltpu.SemaphoreType.DMA((slots, 2)),
            pltpu.SemaphoreType.DMA((seqs, len(spans))),
            pltpu.SemaphoreType.DMA((2, seqs, len(spans))),
        ],
        compiler_params=pltpu.CompilerParams(collective_id=0, has_side_effects=True,
                                             vmem_limit_bytes=40 * 1024 * 1024),
        cost_estimate=pl.CostEstimate(flops=4 * seqs * pos * width * hidden * layers,
                                      bytes_accessed=4 * layers * width * hidden, transcendentals=0),
        name='teacher',
    )(x_t, t_gain, t_w1, t_w2)


def dot_tn(a, b):
    return lax.dot_general(a, b, (((0,), (0,)), ((), ())), preferred_element_type=F32)


def dot_nt(a, b):
    return lax.dot_general(a, b, (((1,), (1,)), ((), ())), preferred_element_type=F32)


def rms_back(dy, x, gain):
    r = inv_rms(x)
    xr = x * r
    gdy = dy * gain
    dx = r * (gdy - xr * jnp.mean(gdy * xr, axis=-1, keepdims=True))
    return dx, jnp.sum(dy * xr, axis=0, keepdims=True)


TILES = 1024
ROW_TILES = 39
W2_AT, W1_AT, SMALL_AT = 234, 624, 1014
SQ_TILE, COUNT_TILE = SMALL_AT + 6, SMALL_AT + 7
PARTS = ((0, W2_AT), (W2_AT, W1_AT - W2_AT), (W1_AT, TILES - W1_AT))


def store_tiles(ref, idx, start, value):
    width = value.shape[1]
    for ct in range(-(-width // 128)):
        lanes = min(128, width - ct * 128)
        piece = value[:, ct * 128:ct * 128 + lanes]
        if lanes < 128:
            piece = jnp.concatenate([piece, jnp.zeros((piece.shape[0], 128 - lanes), F32)], axis=1)
        ref[idx, start + ct * ROW_TILES:start + (ct + 1) * ROW_TILES] = piece.reshape(ROW_TILES, 8, 128)


def store_row(ref, idx, start, row):
    width = row.shape[1]
    for ct in range(-(-width // 128)):
        lanes = min(128, width - ct * 128)
        piece = row[:, ct * 128:ct * 128 + lanes]
        if lanes < 128:
            piece = jnp.concatenate([piece, jnp.zeros((1, 128 - lanes), F32)], axis=1)
        ref[idx, start + ct] = jnp.broadcast_to(piece, (8, 128))


def student_kernel(len_ref, x_ref, feat_ref, w1_ref, w2_ref, g1_ref, g2_ref, proj_ref, out_hbm,
                   grad, recv, s_in, normed_s, pre_s, act_s, dproj_s, send_sem, recv_sem, out_sem):
    core = lax.axis_index('model')
    peer = {'model': 1 - core}
    layers = w1_ref.shape[0]
    pairs = layers // 2
    pos = x_ref.shape[2]
    barrier = pltpu.get_barrier_semaphore()
    pl.semaphore_signal(barrier, inc=1, device_id=peer, device_id_type=MESH)
    pl.semaphore_wait(barrier, 1)
    valid = (lax.broadcasted_iota(jnp.int32, (pos, 1), 0) < len_ref[0]).astype(F32)
    tokens = jnp.broadcast_to(len_ref[0].astype(F32), (8, 128))

    def send(pair, part):
        start, size = PARTS[part]
        return pltpu.make_async_remote_copy(
            grad.at[pairs + pair, pl.ds(start, size)], recv.at[pair, pl.ds(start, size)],
            send_sem.at[pair, part], recv_sem.at[pair, part], device_id=peer, device_id_type=MESH)

    def place(layer):
        pair = lax.div(layer, 2)
        mine = lax.rem(layer, 2) == core
        return pair, mine, jnp.where(mine, pair, pairs + pair)

    def forward(layer, state):
        pair, mine, idx = place(layer)
        s_in[layer] = state
        normed = (state * inv_rms(state) * g1_ref[pl.ds(layer, 1), :]).astype(BF16)
        normed_s[layer] = normed
        pre = jnp.dot(normed, w1_ref[layer], preferred_element_type=F32)
        pre_s[layer] = pre
        act = gelu(pre).astype(BF16)
        act_s[layer] = act
        state = (state + dot_nt(act, w2_ref[layer])).astype(BF16).astype(F32)
        normed_out = (state * inv_rms(state) * g2_ref[pl.ds(layer, 1), :]).astype(BF16)
        err = (jnp.dot(normed_out, proj_ref[layer], preferred_element_type=F32) - feat_ref[layer].astype(F32)) * valid
        sq = jnp.sum(jnp.sum(err * err, axis=0, keepdims=True), axis=1, keepdims=True)
        d_err = err.astype(BF16)
        store_tiles(grad, idx, 0, dot_tn(normed_out, d_err))

        @pl.when(jnp.logical_not(mine))
        def _():
            send(pair, 0).start()

        dx, dg = rms_back(dot_nt(d_err, proj_ref[layer]), state, g2_ref[pl.ds(layer, 1), :])
        dproj_s[layer] = dx
        store_row(grad, idx, SMALL_AT + 3, dg)
        grad[idx, SQ_TILE] = jnp.broadcast_to(sq, (8, 128))
        grad[idx, COUNT_TILE] = tokens
        for spare in range(COUNT_TILE + 1, TILES):
            grad[idx, spare] = jnp.zeros((8, 128), F32)
        return state

    lax.fori_loop(0, layers, forward, x_ref[0].astype(F32).T)

    def backward(step, d_state):
        layer = layers - 1 - step
        pair, mine, idx = place(layer)
        d_state = d_state + dproj_s[layer]
        d_update = d_state.astype(BF16)
        store_tiles(grad, idx, W2_AT, dot_tn(d_update, act_s[layer]))

        @pl.when(jnp.logical_not(mine))
        def _():
            send(pair, 1).start()

        d_act = jnp.dot(d_update, w2_ref[layer], preferred_element_type=F32)
        d_pre = (d_act * gelu_grad(pre_s[layer])).astype(BF16)
        dx, dg = rms_back(dot_nt(d_pre, w1_ref[layer]), s_in[layer], g1_ref[pl.ds(layer, 1), :])
        store_row(grad, idx, SMALL_AT, dg)
        store_tiles(grad, idx, W1_AT, dot_tn(normed_s[layer], d_pre))

        @pl.when(jnp.logical_not(mine))
        def _():
            send(pair, 2).start()

        return d_state + dx

    lax.fori_loop(0, layers, backward, jnp.zeros(s_in.shape[1:], F32))

    def out_copy(pair):
        return pltpu.make_async_copy(grad.at[pair], out_hbm.at[pair], out_sem.at[pair])

    for pair in reversed(range(pairs)):
        for part in range(3):
            send(pair, part).wait_recv()
            start, size = PARTS[part]
            span = pl.ds(start, size)
            grad[pair, span] = grad[pair, span] + recv[pair, span]
        out_copy(pair).start()
    for pair in range(pairs):
        for part in range(3):
            send(pair, part).wait_send()
        out_copy(pair).wait()


def student(x_s, lengths, feats, s_w1, s_w2t, s_gain1, s_gain2, s_proj):
    layers, width, hidden = s_w1.shape
    pos = x_s.shape[2]
    vmem = pl.BlockSpec(memory_space=pltpu.VMEM)
    return pl.pallas_call(
        student_kernel,
        out_shape=jax.ShapeDtypeStruct((layers // 2, TILES, 8, 128), F32),
        in_specs=[pl.BlockSpec(memory_space=pltpu.SMEM)] + [vmem] * 7,
        out_specs=pl.BlockSpec(memory_space=pl.ANY),
        scratch_shapes=[
            pltpu.VMEM((layers, TILES, 8, 128), F32),
            pltpu.VMEM((layers // 2, TILES, 8, 128), F32),
            pltpu.VMEM((layers, pos, width), F32),
            pltpu.VMEM((layers, pos, width), BF16),
            pltpu.VMEM((layers, pos, hidden), F32),
            pltpu.VMEM((layers, pos, hidden), BF16),
            pltpu.VMEM((layers, pos, width), F32),
            pltpu.SemaphoreType.DMA((layers // 2, 3)),
            pltpu.SemaphoreType.DMA((layers // 2, 3)),
            pltpu.SemaphoreType.DMA((layers // 2,)),
        ],
        compiler_params=pltpu.CompilerParams(collective_id=1, has_side_effects=True,
                                             vmem_limit_bytes=67_043_328),
        name='student',
    )(lengths, x_s, feats, s_w1, s_w2t, s_gain1, s_gain2, s_proj)


SUBS = 2
ORDER = ((0, 0), (0, 1), (1, 0), (0, 2), (1, 1), (0, 3), (1, 2), (0, 4), (1, 3), (0, 5), (1, 4), (0, 6), (1, 5), (0, 7),
         (1, 6), (0, 8), (1, 7), (0, 9), (1, 8), (0, 10), (1, 9), (0, 11), (1, 10), (0, 12), (1, 11), (0, 13), (1, 12),
         (1, 13))


def reduce_kernel(side, g_hbm, out_hbm, data, full, near, far,
                  load_sem, rs_send, rs_recv, ag_send, ag_recv, own_sem, d2d_send, d2d_recv):
    core = lax.axis_index('model')
    chip = lax.axis_index('data')
    peer = {'model': 1 - core}
    colors = data.shape[0]
    sub_tiles = TILES // SUBS
    coord = [lax.rem(chip, side), lax.rem(lax.div(chip, side), side), lax.div(chip, side * side)]

    def shifted(axis, by):
        moved = list(coord)
        moved[axis] = lax.rem(coord[axis] + by, side)
        return {'data': (moved[2] * side + moved[1]) * side + moved[0]}

    def load(c, sub):
        span = pl.ds(sub * sub_tiles, sub_tiles)
        return pltpu.make_async_copy(g_hbm.at[c, span], data.at[c, span], load_sem.at[c, sub])

    for sub in range(SUBS):
        for c in range(colors):
            load(c, sub).start()

    barrier = pltpu.get_barrier_semaphore()
    pl.semaphore_signal(barrier, inc=1, device_id=peer, device_id_type=MESH)
    for axis in range(3):
        for by in (1, side - 1):
            pl.semaphore_signal(barrier, inc=1, device_id=shifted(axis, by), device_id_type=MESH)
    pl.semaphore_wait(barrier, 7)

    plus = [shifted(axis, 1) for axis in range(3)]
    minus = [shifted(axis, side - 1) for axis in range(3)]
    sent = []
    emitted = []

    def remote(src, dst, send_sem, recv_sem, axis, upward):
        copy = pltpu.make_async_remote_copy(src, dst, send_sem, recv_sem,
                                            device_id=plus[axis] if upward else minus[axis], device_id_type=MESH)
        copy.start()
        sent.append(copy)
        return copy

    def emit(c, sub, slot, start, count):
        layer = 2 * c + core
        span = pl.ds(start, count)
        k = sub * 7 + slot
        own = pltpu.make_async_copy(full.at[c, span], out_hbm.at[layer, span], own_sem.at[c, k])
        own.start()
        across = pltpu.make_async_remote_copy(
            full.at[c, span], out_hbm.at[layer, span], d2d_send.at[c, k], d2d_recv.at[c, k],
            device_id=peer, device_id_type=MESH)
        across.start()
        emitted.append((own, across))

    def stream(c, sub):
        load(c, sub).wait()
        base = sub * sub_tiles
        bases = []
        near_at, far_at = sub * (near.shape[2] // SUBS), sub * (far.shape[2] // SUBS)
        size = sub_tiles // side
        for phase in range(3):
            half = size // 2
            axis = (c + phase) % 3
            bases.append(base)

            def chunk(by):
                return base + lax.rem(coord[axis] + by, side) * size

            def push(kind, src, dst, upward):
                k = sub * 6 + kind
                return remote(src, dst, rs_send.at[c, phase, k], rs_recv.at[c, phase, k], axis, upward)

            opp, nxt, prv, mine = chunk(2), chunk(1), chunk(3), chunk(0)
            near_span, far_low = pl.ds(near_at, half), pl.ds(far_at, half)
            far_high, far_all = pl.ds(far_at + half, half), pl.ds(far_at, size)
            first_up = push(0, data.at[c, pl.ds(opp, half)], near.at[c, 0, near_span], True)
            first_down = push(1, data.at[c, pl.ds(opp + half, half)], near.at[c, 1, near_span], False)
            early_up = push(2, data.at[c, pl.ds(nxt + half, half)], far.at[c, 0, far_high], True)
            early_down = push(3, data.at[c, pl.ds(prv, half)], far.at[c, 1, far_low], False)
            yield
            first_up.wait_recv()
            span = pl.ds(nxt, half)
            data[c, span] = data[c, span] + near[c, 0, near_span]
            late_up = push(4, data.at[c, span], far.at[c, 0, far_low], True)
            first_down.wait_recv()
            span = pl.ds(prv + half, half)
            data[c, span] = data[c, span] + near[c, 1, near_span]
            late_down = push(5, data.at[c, span], far.at[c, 1, far_high], False)
            yield
            for copy in (early_up, early_down, late_up, late_down):
                copy.wait_recv()
            mine_span = pl.ds(mine, size)
            both = far[c, 0, far_all] + far[c, 1, far_all]
            if phase < 2:
                data[c, mine_span] = data[c, mine_span] + both
            else:
                full[c, mine_span] = data[c, mine_span] + both
            base = mine
            near_at, far_at, size = near_at + half, far_at + size, size // side

        for phase in (2, 1, 0):
            size = sub_tiles // side ** (phase + 1)
            half = size // 2
            axis = (c + phase) % 3
            base = bases[phase]
            last = phase == 0

            def part(by, upper):
                return base + lax.rem(coord[axis] + by, side) * size + (half if upper else 0)

            def spread(kind, start, upward):
                k = sub * 6 + kind
                span = pl.ds(start, half)
                return remote(full.at[c, span], full.at[c, span], ag_send.at[c, phase, k], ag_recv.at[c, phase, k],
                              axis, upward)

            low, high = part(0, False), part(0, True)
            direct = (spread(0, low, True), spread(1, high, False), spread(2, high, True), spread(3, low, False))
            if last:
                emit(c, sub, 0, low, size)
            yield
            direct[0].wait_recv()
            up = spread(4, part(3, False), True)
            direct[1].wait_recv()
            down = spread(5, part(1, True), False)
            if last:
                emit(c, sub, 1, part(3, False), half)
                emit(c, sub, 2, part(1, True), half)
            yield
            direct[2].wait_recv()
            if last:
                emit(c, sub, 3, part(3, True), half)
            direct[3].wait_recv()
            if last:
                emit(c, sub, 4, part(1, False), half)
                yield
            up.wait_recv()
            if last:
                emit(c, sub, 5, part(2, False), half)
            down.wait_recv()
            if last:
                emit(c, sub, 6, part(2, True), half)

    streams = [[stream(c, sub) for c in range(colors)] for sub in range(SUBS)]
    for sub, _ in ORDER:
        for one in streams[sub]:
            next(one, None)

    for copy in sent:
        copy.wait_send()
    for own, across in emitted:
        own.wait()
        across.wait()


def reduce_all(grads, side):
    colors = grads.shape[0]
    hbm = pl.BlockSpec(memory_space=pl.ANY)
    return pl.pallas_call(
        functools.partial(reduce_kernel, side),
        out_shape=jax.ShapeDtypeStruct((2 * colors, TILES, 8, 128), F32),
        in_specs=[hbm],
        out_specs=hbm,
        scratch_shapes=[
            pltpu.VMEM((colors, TILES, 8, 128), F32),
            pltpu.VMEM((colors, TILES, 8, 128), F32),
            pltpu.VMEM((colors, 2, 168, 8, 128), F32),
            pltpu.VMEM((colors, 2, 336, 8, 128), F32),
            pltpu.SemaphoreType.DMA((colors, SUBS)),
            pltpu.SemaphoreType.DMA((colors, 3, 6 * SUBS)),
            pltpu.SemaphoreType.DMA((colors, 3, 6 * SUBS)),
            pltpu.SemaphoreType.DMA((colors, 3, 6 * SUBS)),
            pltpu.SemaphoreType.DMA((colors, 3, 6 * SUBS)),
            pltpu.SemaphoreType.DMA((colors, 7 * SUBS)),
            pltpu.SemaphoreType.DMA((colors, 7 * SUBS)),
            pltpu.SemaphoreType.DMA((colors, 7 * SUBS)),
        ],
        compiler_params=pltpu.CompilerParams(collective_id=2, has_side_effects=True,
                                             vmem_limit_bytes=56 * 1024 * 1024),
        name='reduce_all',
    )(grads)


def finish_kernel(terms, flat_ref, loss_ref, gw1_ref, gw2_ref, gg1_ref, gg2_ref, gproj_ref):
    layer = pl.program_id(0)
    inv = 1.0 / (terms * flat_ref[0, COUNT_TILE, 0:1, 0:1])
    two = 2.0 * inv

    def unpack(ref, start, rows):
        width = ref.shape[2]
        for ct in range(-(-width // 128)):
            lanes = min(128, width - ct * 128)
            piece = flat_ref[0, start + ct * ROW_TILES:start + (ct + 1) * ROW_TILES].reshape(rows, 128) * two
            ref[0, :, ct * 128:ct * 128 + lanes] = piece[:, :lanes]

    unpack(gproj_ref, 0, gproj_ref.shape[1])
    unpack(gw2_ref, W2_AT, gw2_ref.shape[1])
    unpack(gw1_ref, W1_AT, gw1_ref.shape[1])
    for ref, start in ((gg1_ref, SMALL_AT), (gg2_ref, SMALL_AT + 3)):
        width = ref.shape[1]
        for ct in range(-(-width // 128)):
            lanes = min(128, width - ct * 128)
            cols = slice(ct * 128, ct * 128 + lanes)
            row = flat_ref[0, start + ct, 0:1, 0:lanes] * two
            here = lax.broadcasted_iota(jnp.int32, (ref.shape[0], lanes), 0) == layer
            ref[:, cols] = jnp.where(here, row, ref[:, cols])

    @pl.when(layer == 0)
    def _():
        loss_ref[...] = jnp.zeros_like(loss_ref)

    loss_ref[...] += flat_ref[0, SQ_TILE, 0:1, 0:1] * inv


def finish(flat, width, hidden, t_width):
    layers = flat.shape[0]
    per_layer = lambda a, b: pl.BlockSpec((1, a, b), lambda l: (l, 0, 0))
    whole = lambda a, b: pl.BlockSpec((a, b), lambda l: (0, 0))
    return pl.pallas_call(
        functools.partial(finish_kernel, float(layers * t_width)),
        grid=(layers,),
        out_shape=(jax.ShapeDtypeStruct((1, 1), F32),
                   jax.ShapeDtypeStruct((layers, width, hidden), F32),
                   jax.ShapeDtypeStruct((layers, width, hidden), F32),
                   jax.ShapeDtypeStruct((layers, width), F32),
                   jax.ShapeDtypeStruct((layers, width), F32),
                   jax.ShapeDtypeStruct((layers, width, t_width), F32)),
        in_specs=[pl.BlockSpec((1, TILES, 8, 128), lambda l: (l, 0, 0, 0))],
        out_specs=(whole(1, 1), per_layer(width, hidden), per_layer(width, hidden),
                   whole(layers, width), whole(layers, width), per_layer(width, t_width)),
        compiler_params=pltpu.CompilerParams(vmem_limit_bytes=48 * 1024 * 1024),
        name='finish',
    )(flat)


def solution(mesh):
    side = round(mesh.shape['data'] ** (1 / 3))

    def body(x_t, x_s, lengths, t_w1, t_w2, t_gain, s_w1, s_w2, s_gain1, s_gain2, s_proj):
        layers, width, hidden = s_w1.shape
        feats = teacher(x_t, t_w1, t_w2, t_gain, layers)
        grads = student(jnp.swapaxes(x_s, 1, 2), lengths, feats, s_w1, jnp.swapaxes(s_w2, 1, 2),
                        s_gain1, s_gain2, s_proj)
        flat = reduce_all(grads, side)
        loss, gw1, gw2, gg1, gg2, gproj = finish(flat, width, hidden, x_t.shape[2])
        return loss[0, 0], gw1, jnp.swapaxes(gw2, 1, 2), gg1, gg2, gproj

    in_specs = (P('data', 'model', None), P(ALL_AXES, None, None), P(ALL_AXES),
                P(None, None, 'model'), P(None, 'model', None), P(), P(), P(), P(), P(), P())
    out_specs = (P(), P(), P(), P(), P(), P())
    return jax.shard_map(body, mesh=mesh, in_specs=in_specs, out_specs=out_specs, check_vma=False)
```

```python
import functools

import jax
import jax.numpy as jnp
from jax import lax
from jax.experimental import pallas as pl
from jax.experimental.pallas import tpu as pltpu
from jax.sharding import PartitionSpec as P

RMS_EPS = 1e-6
ALL_AXES = ('data', 'model')
MESH = pl.DeviceIdType.MESH
GELU_C = 0.7978845608028654
GELU_A = 0.044715
F32 = jnp.float32
BF16 = jnp.bfloat16


def gelu(x):
    half = 0.5 * x
    return half + half * jnp.tanh(x * (GELU_C + (GELU_C * GELU_A) * (x * x)))


def gelu_grad(x):
    sq = x * x
    t = jnp.tanh(GELU_C * (x + GELU_A * (sq * x)))
    return 0.5 * (1.0 + t) + (0.5 * x) * (1.0 - t * t) * (GELU_C * (1.0 + (3.0 * GELU_A) * sq))


def inv_rms(wide):
    return lax.rsqrt(jnp.mean(wide * wide, axis=-1, keepdims=True) + RMS_EPS)


def teacher_kernel(layers, per_group, spans, k_chunks, x_ref, gain_ref, w1_hbm, w2_hbm, feat_ref,
                   xbuf, hbuf, part, recv, w1buf, w2buf,
                   x_send, x_recv, w_sem, p_send, p_recv):
    core = lax.axis_index('model')
    peer = {'model': 1 - core}
    seqs, pos, width = hbuf.shape
    slots, _, hidden = w1buf.shape
    blocks, out_w = part.shape[1], part.shape[3]
    step = hidden // k_chunks

    def fetch(layer, slot):
        return (pltpu.make_async_copy(w1_hbm.at[layer], w1buf.at[slot], w_sem.at[slot, 0]),
                pltpu.make_async_copy(w2_hbm.at[layer], w2buf.at[slot], w_sem.at[slot, 1]))

    for layer in range(slots - 1):
        for copy in fetch(layer, layer):
            copy.start()

    barrier = pltpu.get_barrier_semaphore()
    pl.semaphore_signal(barrier, inc=1, device_id=peer, device_id_type=MESH)
    part[...] = jnp.zeros(part.shape, F32)
    recv[1] = jnp.zeros(recv.shape[1:], F32)
    xbuf[core] = x_ref[...]
    pl.semaphore_wait(barrier, 1)

    x_copy = pltpu.make_async_remote_copy(x_ref, xbuf.at[core], x_send, x_recv, device_id=peer, device_id_type=MESH)
    x_copy.start()
    x_copy.wait()
    for seq in range(seqs):
        for c in range(2):
            hbuf[seq, c * (pos // 2):(c + 1) * (pos // 2), :] = xbuf[c, seq]

    def exchange(seq, slot, k):
        span = pl.ds(*spans[k])
        return pltpu.make_async_remote_copy(
            part.at[seq, span], recv.at[slot, seq, span], p_send.at[seq, k], p_recv.at[slot, seq, k],
            device_id=peer, device_id_type=MESH)

    def absorb(seq, slot):
        update = jnp.concatenate([part[seq, b] + recv[slot, seq, b] for b in range(blocks)], axis=1)
        state = (hbuf[seq].astype(F32) + update).astype(BF16)
        hbuf[seq] = state
        return state.astype(F32)

    def block(layer, _):
        slot = lax.rem(layer, slots)

        @pl.when(layer + (slots - 1) < layers)
        def _():
            for copy in fetch(layer + (slots - 1), lax.rem(layer + (slots - 1), slots)):
                copy.start()

        for seq in range(seqs):
            old = lax.rem(layer + 1, 2)
            if seq == 0:
                for copy in fetch(layer, slot):
                    copy.wait()

            @pl.when(layer > 0)
            def _():
                for k in range(len(spans)):
                    exchange(seq, old, k).wait()

            wide = absorb(seq, old)
            normed = (wide * inv_rms(wide) * gain_ref[pl.ds(layer, 1), :]).astype(BF16)
            acc = [None] * len(spans)
            for c in range(k_chunks):
                pre = jnp.dot(normed, w1buf[slot, :, c * step:(c + 1) * step], preferred_element_type=F32)
                act = gelu(pre).astype(BF16)
                for k, (first, count) in enumerate(spans):
                    cols = slice(first * out_w, (first + count) * out_w)
                    term = jnp.dot(act, w2buf[slot, c * step:(c + 1) * step, cols], preferred_element_type=F32)
                    acc[k] = term if acc[k] is None else acc[k] + term
                    if c == k_chunks - 1:
                        for b in range(count):
                            part[seq, first + b] = acc[k][:, b * out_w:(b + 1) * out_w]
                        exchange(seq, lax.rem(layer, 2), k).start()

        @pl.when((layer > 0) & (lax.rem(layer, per_group) == 0))
        def _():
            feat_ref[lax.div(layer, per_group) - 1] = hbuf[core]
        return 0

    lax.fori_loop(0, layers, block, 0)
    for seq in range(seqs):
        for k in range(len(spans)):
            exchange(seq, (layers - 1) % 2, k).wait()
        absorb(seq, (layers - 1) % 2)
    feat_ref[layers // per_group - 1] = hbuf[core]


def teacher(x_t, t_w1, t_w2, t_gain, n_feat):
    layers, width, hidden = t_w1.shape
    seqs, half_pos, _ = x_t.shape
    pos = 2 * half_pos
    slots, blocks = 3, 3
    out_w = width // blocks
    spans = ((0, 1), (1, 2))
    vmem = pl.BlockSpec(memory_space=pltpu.VMEM)
    hbm = pl.BlockSpec(memory_space=pl.ANY)
    return pl.pallas_call(
        functools.partial(teacher_kernel, layers, layers // n_feat, spans, 1),
        out_shape=jax.ShapeDtypeStruct((n_feat, pos, width), BF16),
        in_specs=[vmem, vmem, hbm, hbm],
        out_specs=vmem,
        scratch_shapes=[
            pltpu.VMEM((2, seqs, half_pos, width), BF16),
            pltpu.VMEM((seqs, pos, width), BF16),
            pltpu.VMEM((seqs, blocks, pos, out_w), F32),
            pltpu.VMEM((2, seqs, blocks, pos, out_w), F32),
            pltpu.VMEM((slots, width, hidden), BF16),
            pltpu.VMEM((slots, hidden, width), BF16),
            pltpu.SemaphoreType.DMA,
            pltpu.SemaphoreType.DMA,
            pltpu.SemaphoreType.DMA((slots, 2)),
            pltpu.SemaphoreType.DMA((seqs, len(spans))),
            pltpu.SemaphoreType.DMA((2, seqs, len(spans))),
        ],
        compiler_params=pltpu.CompilerParams(collective_id=0, has_side_effects=True,
                                             vmem_limit_bytes=40 * 1024 * 1024),
        cost_estimate=pl.CostEstimate(flops=4 * seqs * pos * width * hidden * layers,
                                      bytes_accessed=4 * layers * width * hidden, transcendentals=0),
        name='teacher',
    )(x_t, t_gain, t_w1, t_w2)


def dot_tn(a, b):
    return lax.dot_general(a, b, (((0,), (0,)), ((), ())), preferred_element_type=F32)


def dot_nt(a, b):
    return lax.dot_general(a, b, (((1,), (1,)), ((), ())), preferred_element_type=F32)


def rms_back(dy, x, gain):
    r = inv_rms(x)
    xr = x * r
    gdy = dy * gain
    dx = r * (gdy - xr * jnp.mean(gdy * xr, axis=-1, keepdims=True))
    return dx, jnp.sum(dy * xr, axis=0, keepdims=True)


TILES = 1024
ROW_TILES = 39
W2_AT, W1_AT, SMALL_AT = 234, 624, 1014
SQ_TILE, COUNT_TILE = SMALL_AT + 6, SMALL_AT + 7
PARTS = ((0, W2_AT), (W2_AT, W1_AT - W2_AT), (W1_AT, TILES - W1_AT))


def store_tiles(ref, idx, start, value):
    width = value.shape[1]
    for ct in range(-(-width // 128)):
        lanes = min(128, width - ct * 128)
        piece = value[:, ct * 128:ct * 128 + lanes]
        if lanes < 128:
            piece = jnp.concatenate([piece, jnp.zeros((piece.shape[0], 128 - lanes), F32)], axis=1)
        ref[idx, start + ct * ROW_TILES:start + (ct + 1) * ROW_TILES] = piece.reshape(ROW_TILES, 8, 128)


def store_row(ref, idx, start, row):
    width = row.shape[1]
    for ct in range(-(-width // 128)):
        lanes = min(128, width - ct * 128)
        piece = row[:, ct * 128:ct * 128 + lanes]
        if lanes < 128:
            piece = jnp.concatenate([piece, jnp.zeros((1, 128 - lanes), F32)], axis=1)
        ref[idx, start + ct] = jnp.broadcast_to(piece, (8, 128))


def student_kernel(len_ref, x_ref, g1_ref, g2_ref, feat_hbm, w1_hbm, w2_hbm, proj_hbm, out_hbm,
                   grad, recv, s_in, normed_s, pre_s, act_s, dproj_s, feat_ref, w1_ref, w2_ref, proj_ref,
                   in_sem, send_sem, recv_sem, out_sem):
    core = lax.axis_index('model')
    peer = {'model': 1 - core}
    layers = w1_ref.shape[0]

    def fetch(layer):
        pairs_of = ((w1_hbm, w1_ref), (w2_hbm, w2_ref), (proj_hbm, proj_ref), (feat_hbm, feat_ref))
        return [pltpu.make_async_copy(src.at[layer], dst.at[layer], in_sem.at[layer, k])
                for k, (src, dst) in enumerate(pairs_of)]

    for layer in range(layers):
        for copy in fetch(layer):
            copy.start()
    pairs = layers // 2
    pos = x_ref.shape[2]
    barrier = pltpu.get_barrier_semaphore()
    pl.semaphore_signal(barrier, inc=1, device_id=peer, device_id_type=MESH)
    pl.semaphore_wait(barrier, 1)
    valid = (lax.broadcasted_iota(jnp.int32, (pos, 1), 0) < len_ref[0]).astype(F32)
    tokens = jnp.broadcast_to(len_ref[0].astype(F32), (8, 128))

    def send(pair, part):
        start, size = PARTS[part]
        return pltpu.make_async_remote_copy(
            grad.at[pairs + pair, pl.ds(start, size)], recv.at[pair, pl.ds(start, size)],
            send_sem.at[pair, part], recv_sem.at[pair, part], device_id=peer, device_id_type=MESH)

    def place(layer):
        pair = lax.div(layer, 2)
        mine = lax.rem(layer, 2) == core
        return pair, mine, jnp.where(mine, pair, pairs + pair)

    def forward(layer, state):
        pair, mine, idx = place(layer)
        for copy in fetch(layer):
            copy.wait()
        s_in[layer] = state
        normed = (state * inv_rms(state) * g1_ref[pl.ds(layer, 1), :]).astype(BF16)
        normed_s[layer] = normed
        pre = jnp.dot(normed, w1_ref[layer], preferred_element_type=F32)
        pre_s[layer] = pre
        act = gelu(pre).astype(BF16)
        act_s[layer] = act
        state = (state + dot_nt(act, w2_ref[layer])).astype(BF16).astype(F32)
        normed_out = (state * inv_rms(state) * g2_ref[pl.ds(layer, 1), :]).astype(BF16)
        err = (jnp.dot(normed_out, proj_ref[layer], preferred_element_type=F32) - feat_ref[layer].astype(F32)) * valid
        sq = jnp.sum(jnp.sum(err * err, axis=0, keepdims=True), axis=1, keepdims=True)
        d_err = err.astype(BF16)
        store_tiles(grad, idx, 0, dot_tn(normed_out, d_err))

        @pl.when(jnp.logical_not(mine))
        def _():
            send(pair, 0).start()

        dx, dg = rms_back(dot_nt(d_err, proj_ref[layer]), state, g2_ref[pl.ds(layer, 1), :])
        dproj_s[layer] = dx
        store_row(grad, idx, SMALL_AT + 3, dg)
        grad[idx, SQ_TILE] = jnp.broadcast_to(sq, (8, 128))
        grad[idx, COUNT_TILE] = tokens
        for spare in range(COUNT_TILE + 1, TILES):
            grad[idx, spare] = jnp.zeros((8, 128), F32)
        return state

    lax.fori_loop(0, layers, forward, x_ref[0].astype(F32).T)

    def backward(step, d_state):
        layer = layers - 1 - step
        pair, mine, idx = place(layer)
        d_state = d_state + dproj_s[layer]
        d_update = d_state.astype(BF16)
        store_tiles(grad, idx, W2_AT, dot_tn(d_update, act_s[layer]))

        @pl.when(jnp.logical_not(mine))
        def _():
            send(pair, 1).start()

        d_act = jnp.dot(d_update, w2_ref[layer], preferred_element_type=F32)
        d_pre = (d_act * gelu_grad(pre_s[layer])).astype(BF16)
        dx, dg = rms_back(dot_nt(d_pre, w1_ref[layer]), s_in[layer], g1_ref[pl.ds(layer, 1), :])
        store_row(grad, idx, SMALL_AT, dg)
        store_tiles(grad, idx, W1_AT, dot_tn(normed_s[layer], d_pre))

        @pl.when(jnp.logical_not(mine))
        def _():
            send(pair, 2).start()

        return d_state + dx

    lax.fori_loop(0, layers, backward, jnp.zeros(s_in.shape[1:], F32))

    def out_copy(pair, part):
        span = pl.ds(*PARTS[part])
        return pltpu.make_async_copy(grad.at[pair, span], out_hbm.at[pair, span], out_sem.at[pair, part])

    for pair in reversed(range(pairs)):
        for part in range(3):
            send(pair, part).wait_recv()
            start, size = PARTS[part]
            span = pl.ds(start, size)
            grad[pair, span] = grad[pair, span] + recv[pair, span]
            out_copy(pair, part).start()
    for pair in range(pairs):
        for part in range(3):
            send(pair, part).wait_send()
            out_copy(pair, part).wait()


def student(x_s, lengths, feats, s_w1, s_w2t, s_gain1, s_gain2, s_proj):
    layers, width, hidden = s_w1.shape
    pos = x_s.shape[2]
    vmem = pl.BlockSpec(memory_space=pltpu.VMEM)
    return pl.pallas_call(
        student_kernel,
        out_shape=jax.ShapeDtypeStruct((layers // 2, TILES, 8, 128), F32),
        in_specs=[pl.BlockSpec(memory_space=pltpu.SMEM)] + [vmem] * 3 + [pl.BlockSpec(memory_space=pl.ANY)] * 4,
        out_specs=pl.BlockSpec(memory_space=pl.ANY),
        scratch_shapes=[
            pltpu.VMEM((layers, TILES, 8, 128), F32),
            pltpu.VMEM((layers // 2, TILES, 8, 128), F32),
            pltpu.VMEM((layers, pos, width), F32),
            pltpu.VMEM((layers, pos, width), BF16),
            pltpu.VMEM((layers, pos, hidden), F32),
            pltpu.VMEM((layers, pos, hidden), BF16),
            pltpu.VMEM((layers, pos, width), F32),
            pltpu.VMEM(feats.shape, BF16),
            pltpu.VMEM(s_w1.shape, BF16),
            pltpu.VMEM(s_w2t.shape, BF16),
            pltpu.VMEM(s_proj.shape, BF16),
            pltpu.SemaphoreType.DMA((layers, 4)),
            pltpu.SemaphoreType.DMA((layers // 2, 3)),
            pltpu.SemaphoreType.DMA((layers // 2, 3)),
            pltpu.SemaphoreType.DMA((layers // 2, 3)),
        ],
        compiler_params=pltpu.CompilerParams(collective_id=1, has_side_effects=True,
                                             vmem_limit_bytes=67_043_328),
        name='student',
    )(lengths, x_s, s_gain1, s_gain2, feats, s_w1, s_w2t, s_proj)


SUBS = 2
ORDER = ((0, 0), (0, 1), (1, 0), (0, 2), (1, 1), (0, 3), (1, 2), (0, 4), (1, 3), (0, 5), (1, 4), (0, 6), (1, 5), (0, 7),
         (1, 6), (0, 8), (1, 7), (0, 9), (1, 8), (0, 10), (1, 9), (0, 11), (1, 10), (0, 12), (1, 11), (0, 13), (1, 12),
         (1, 13))


def reduce_kernel(side, g_hbm, out_hbm, data, full, near, far,
                  load_sem, rs_send, rs_recv, ag_send, ag_recv, own_sem, d2d_send, d2d_recv):
    core = lax.axis_index('model')
    chip = lax.axis_index('data')
    peer = {'model': 1 - core}
    colors = data.shape[0]
    sub_tiles = TILES // SUBS
    coord = [lax.rem(chip, side), lax.rem(lax.div(chip, side), side), lax.div(chip, side * side)]

    def shifted(axis, by):
        moved = list(coord)
        moved[axis] = lax.rem(coord[axis] + by, side)
        return {'data': (moved[2] * side + moved[1]) * side + moved[0]}

    def load(c, sub):
        span = pl.ds(sub * sub_tiles, sub_tiles)
        return pltpu.make_async_copy(g_hbm.at[c, span], data.at[c, span], load_sem.at[c, sub])

    for sub in range(SUBS):
        for c in range(colors):
            load(c, sub).start()

    barrier = pltpu.get_barrier_semaphore()
    pl.semaphore_signal(barrier, inc=1, device_id=peer, device_id_type=MESH)
    for axis in range(3):
        for by in (1, side - 1):
            pl.semaphore_signal(barrier, inc=1, device_id=shifted(axis, by), device_id_type=MESH)
    pl.semaphore_wait(barrier, 7)

    plus = [shifted(axis, 1) for axis in range(3)]
    minus = [shifted(axis, side - 1) for axis in range(3)]
    sent = []
    emitted = []

    def remote(src, dst, send_sem, recv_sem, axis, upward):
        copy = pltpu.make_async_remote_copy(src, dst, send_sem, recv_sem,
                                            device_id=plus[axis] if upward else minus[axis], device_id_type=MESH)
        copy.start()
        sent.append(copy)
        return copy

    def emit(c, sub, slot, start, count):
        layer = 2 * c + core
        span = pl.ds(start, count)
        k = sub * 7 + slot
        own = pltpu.make_async_copy(full.at[c, span], out_hbm.at[layer, span], own_sem.at[c, k])
        own.start()
        across = pltpu.make_async_remote_copy(
            full.at[c, span], out_hbm.at[layer, span], d2d_send.at[c, k], d2d_recv.at[c, k],
            device_id=peer, device_id_type=MESH)
        across.start()
        emitted.append((own, across))

    def stream(c, sub):
        load(c, sub).wait()
        base = sub * sub_tiles
        bases = []
        near_at, far_at = sub * (near.shape[2] // SUBS), sub * (far.shape[2] // SUBS)
        size = sub_tiles // side
        for phase in range(3):
            half = size // 2
            axis = (c + phase) % 3
            bases.append(base)

            def chunk(by):
                return base + lax.rem(coord[axis] + by, side) * size

            def push(kind, src, dst, upward):
                k = sub * 6 + kind
                return remote(src, dst, rs_send.at[c, phase, k], rs_recv.at[c, phase, k], axis, upward)

            opp, nxt, prv, mine = chunk(2), chunk(1), chunk(3), chunk(0)
            near_span, far_low = pl.ds(near_at, half), pl.ds(far_at, half)
            far_high, far_all = pl.ds(far_at + half, half), pl.ds(far_at, size)
            first_up = push(0, data.at[c, pl.ds(opp, half)], near.at[c, 0, near_span], True)
            first_down = push(1, data.at[c, pl.ds(opp + half, half)], near.at[c, 1, near_span], False)
            early_up = push(2, data.at[c, pl.ds(nxt + half, half)], far.at[c, 0, far_high], True)
            early_down = push(3, data.at[c, pl.ds(prv, half)], far.at[c, 1, far_low], False)
            yield
            first_up.wait_recv()
            span = pl.ds(nxt, half)
            data[c, span] = data[c, span] + near[c, 0, near_span]
            late_up = push(4, data.at[c, span], far.at[c, 0, far_low], True)
            first_down.wait_recv()
            span = pl.ds(prv + half, half)
            data[c, span] = data[c, span] + near[c, 1, near_span]
            late_down = push(5, data.at[c, span], far.at[c, 1, far_high], False)
            yield
            for copy in (early_up, early_down, late_up, late_down):
                copy.wait_recv()
            mine_span = pl.ds(mine, size)
            both = far[c, 0, far_all] + far[c, 1, far_all]
            if phase < 2:
                data[c, mine_span] = data[c, mine_span] + both
            else:
                full[c, mine_span] = data[c, mine_span] + both
            base = mine
            near_at, far_at, size = near_at + half, far_at + size, size // side

        for phase in (2, 1, 0):
            size = sub_tiles // side ** (phase + 1)
            half = size // 2
            axis = (c + phase) % 3
            base = bases[phase]
            last = phase == 0

            def part(by, upper):
                return base + lax.rem(coord[axis] + by, side) * size + (half if upper else 0)

            def spread(kind, start, upward):
                k = sub * 6 + kind
                span = pl.ds(start, half)
                return remote(full.at[c, span], full.at[c, span], ag_send.at[c, phase, k], ag_recv.at[c, phase, k],
                              axis, upward)

            low, high = part(0, False), part(0, True)
            direct = (spread(0, low, True), spread(1, high, False), spread(2, high, True), spread(3, low, False))
            if last:
                emit(c, sub, 0, low, size)
            yield
            direct[0].wait_recv()
            up = spread(4, part(3, False), True)
            direct[1].wait_recv()
            down = spread(5, part(1, True), False)
            if last:
                emit(c, sub, 1, part(3, False), half)
                emit(c, sub, 2, part(1, True), half)
            yield
            direct[2].wait_recv()
            if last:
                emit(c, sub, 3, part(3, True), half)
            direct[3].wait_recv()
            if last:
                emit(c, sub, 4, part(1, False), half)
                yield
            up.wait_recv()
            if last:
                emit(c, sub, 5, part(2, False), half)
            down.wait_recv()
            if last:
                emit(c, sub, 6, part(2, True), half)

    streams = [[stream(c, sub) for c in range(colors)] for sub in range(SUBS)]
    for sub, _ in ORDER:
        for one in streams[sub]:
            next(one, None)

    for copy in sent:
        copy.wait_send()
    for own, across in emitted:
        own.wait()
        across.wait()


def reduce_all(grads, side):
    colors = grads.shape[0]
    hbm = pl.BlockSpec(memory_space=pl.ANY)
    return pl.pallas_call(
        functools.partial(reduce_kernel, side),
        out_shape=jax.ShapeDtypeStruct((2 * colors, TILES, 8, 128), F32),
        in_specs=[hbm],
        out_specs=hbm,
        scratch_shapes=[
            pltpu.VMEM((colors, TILES, 8, 128), F32),
            pltpu.VMEM((colors, TILES, 8, 128), F32),
            pltpu.VMEM((colors, 2, 168, 8, 128), F32),
            pltpu.VMEM((colors, 2, 336, 8, 128), F32),
            pltpu.SemaphoreType.DMA((colors, SUBS)),
            pltpu.SemaphoreType.DMA((colors, 3, 6 * SUBS)),
            pltpu.SemaphoreType.DMA((colors, 3, 6 * SUBS)),
            pltpu.SemaphoreType.DMA((colors, 3, 6 * SUBS)),
            pltpu.SemaphoreType.DMA((colors, 3, 6 * SUBS)),
            pltpu.SemaphoreType.DMA((colors, 7 * SUBS)),
            pltpu.SemaphoreType.DMA((colors, 7 * SUBS)),
            pltpu.SemaphoreType.DMA((colors, 7 * SUBS)),
        ],
        compiler_params=pltpu.CompilerParams(collective_id=2, has_side_effects=True,
                                             vmem_limit_bytes=56 * 1024 * 1024),
        name='reduce_all',
    )(grads)


def finish_kernel(terms, flat_ref, loss_ref, gw1_ref, gw2_ref, gg1_ref, gg2_ref, gproj_ref):
    layer = pl.program_id(0)
    inv = 1.0 / (terms * flat_ref[0, COUNT_TILE, 0:1, 0:1])
    two = 2.0 * inv

    def unpack(ref, start, rows):
        width = ref.shape[2]
        for ct in range(-(-width // 128)):
            lanes = min(128, width - ct * 128)
            piece = flat_ref[0, start + ct * ROW_TILES:start + (ct + 1) * ROW_TILES].reshape(rows, 128) * two
            ref[0, :, ct * 128:ct * 128 + lanes] = piece[:, :lanes]

    unpack(gproj_ref, 0, gproj_ref.shape[1])
    unpack(gw2_ref, W2_AT, gw2_ref.shape[1])
    unpack(gw1_ref, W1_AT, gw1_ref.shape[1])
    for ref, start in ((gg1_ref, SMALL_AT), (gg2_ref, SMALL_AT + 3)):
        width = ref.shape[1]
        for ct in range(-(-width // 128)):
            lanes = min(128, width - ct * 128)
            cols = slice(ct * 128, ct * 128 + lanes)
            row = flat_ref[0, start + ct, 0:1, 0:lanes] * two
            here = lax.broadcasted_iota(jnp.int32, (ref.shape[0], lanes), 0) == layer
            ref[:, cols] = jnp.where(here, row, ref[:, cols])

    @pl.when(layer == 0)
    def _():
        loss_ref[...] = jnp.zeros_like(loss_ref)

    loss_ref[...] += flat_ref[0, SQ_TILE, 0:1, 0:1] * inv


def finish(flat, width, hidden, t_width):
    layers = flat.shape[0]
    per_layer = lambda a, b: pl.BlockSpec((1, a, b), lambda l: (l, 0, 0))
    whole = lambda a, b: pl.BlockSpec((a, b), lambda l: (0, 0))
    return pl.pallas_call(
        functools.partial(finish_kernel, float(layers * t_width)),
        grid=(layers,),
        out_shape=(jax.ShapeDtypeStruct((1, 1), F32),
                   jax.ShapeDtypeStruct((layers, width, hidden), F32),
                   jax.ShapeDtypeStruct((layers, width, hidden), F32),
                   jax.ShapeDtypeStruct((layers, width), F32),
                   jax.ShapeDtypeStruct((layers, width), F32),
                   jax.ShapeDtypeStruct((layers, width, t_width), F32)),
        in_specs=[pl.BlockSpec((1, TILES, 8, 128), lambda l: (l, 0, 0, 0))],
        out_specs=(whole(1, 1), per_layer(width, hidden), per_layer(width, hidden),
                   whole(layers, width), whole(layers, width), per_layer(width, t_width)),
        compiler_params=pltpu.CompilerParams(vmem_limit_bytes=48 * 1024 * 1024),
        name='finish',
    )(flat)


def solution(mesh):
    side = round(mesh.shape['data'] ** (1 / 3))

    def body(x_t, x_s, lengths, t_w1, t_w2, t_gain, s_w1, s_w2, s_gain1, s_gain2, s_proj):
        layers, width, hidden = s_w1.shape
        feats = teacher(x_t, t_w1, t_w2, t_gain, layers)
        grads = student(jnp.swapaxes(x_s, 1, 2), lengths, feats, s_w1, jnp.swapaxes(s_w2, 1, 2),
                        s_gain1, s_gain2, s_proj)
        flat = reduce_all(grads, side)
        loss, gw1, gw2, gg1, gg2, gproj = finish(flat, width, hidden, x_t.shape[2])
        return loss[0, 0], gw1, jnp.swapaxes(gw2, 1, 2), gg1, gg2, gproj

    in_specs = (P('data', 'model', None), P(ALL_AXES, None, None), P(ALL_AXES),
                P(None, None, 'model'), P(None, 'model', None), P(), P(), P(), P(), P(), P())
    out_specs = (P(), P(), P(), P(), P(), P())
    return jax.shard_map(body, mesh=mesh, in_specs=in_specs, out_specs=out_specs, check_vma=False)
```
